128 devices in a mesh: dp: 1, ep: 64 (over z, y, x), tp: 2 (over core).
Axes of the slice: x: 4, y: 4, z: 4, core: 2. Of those that a mesh axis runs over, the one named last changes fastest.
Arguments:
- x_in: bfloat16 [65536, 896], P(('dp', 'ep'))
- expert_ids: int32 [65536, 8], P(('dp', 'ep'))
- gate_vals: float32 [65536, 8], P(('dp', 'ep'))
- w_gate: bfloat16 [64, 896, 2560], P('ep', None, 'tp')
- w_up: bfloat16 [64, 896, 2560], P('ep', None, 'tp')
- w_down: bfloat16 [64, 2560, 896], P('ep', 'tp')
Outputs:
- output: bfloat16 [65536, 896], P(('dp', 'ep'))
All inputs are finite; a program needn't handle non-finite values.
Results may differ from the reference program's by a relative error of at most 0.0107107.
Values are sent between devices in bfloat16 or wider.
A program may use at most 1 GiB of HBM per device.

```python
import jax
import jax.numpy as jnp
from jax import lax

D = 896
FF = 2560
EXPERTS = 64
TOP = 8
TOKENS = 1024
SOURCES = 64

CAPACITY = (5 * TOP * TOKENS) // (4 * EXPERTS)


def draw_routing(key, num_rows):
    scores = jax.random.randint(key, (num_rows, EXPERTS), 0, 1048576, dtype=jnp.int32)
    scores = scores * EXPERTS + jnp.arange(EXPERTS, dtype=jnp.int32)[None, :]
    _, chosen = lax.top_k(scores, TOP)
    return chosen.astype(jnp.int32)


def setup_inputs(seed: int = 0, part: int = 0) -> dict:
    base = jax.random.key(seed)
    key_x, key_ids, key_gate = jax.random.split(jax.random.fold_in(base, part), 3)
    key_wg, key_wu, key_wd = jax.random.split(jax.random.key(seed + 1), 3)
    num_rows = SOURCES * TOKENS
    x_in = jax.random.normal(key_x, (num_rows, D), jnp.float32).astype(jnp.bfloat16)
    expert_ids = draw_routing(key_ids, num_rows)
    gate_vals = jax.random.uniform(key_gate, (num_rows, TOP), jnp.float32, 0.25, 1.25)
    w_gate = (jax.random.normal(key_wg, (EXPERTS, D, FF), jnp.float32) * D ** -0.5).astype(jnp.bfloat16)
    w_up = (jax.random.normal(key_wu, (EXPERTS, D, FF), jnp.float32) * D ** -0.5).astype(jnp.bfloat16)
    w_down = (jax.random.normal(key_wd, (EXPERTS, FF, D), jnp.float32) * FF ** -0.5).astype(jnp.bfloat16)
    return {'x_in': x_in, 'expert_ids': expert_ids, 'gate_vals': gate_vals,
            'w_gate': w_gate, 'w_up': w_up, 'w_down': w_down}


def slot_numbers(ids_one):
    flat_ids = ids_one.reshape(TOKENS * TOP)
    onehot = (flat_ids[:, None] == jnp.arange(EXPERTS, dtype=jnp.int32)[None, :]).astype(jnp.int32)
    slots = jnp.sum((jnp.cumsum(onehot, axis=0) - onehot) * onehot, axis=1)
    return slots.reshape(TOKENS, TOP)


def reference(x_in, expert_ids, gate_vals, w_gate, w_up, w_down):
    x_src = x_in.reshape(SOURCES, TOKENS, D)
    ids_src = expert_ids.reshape(SOURCES, TOKENS, TOP)
    gates_src = gate_vals.reshape(SOURCES, TOKENS, TOP)
    slots = lax.map(slot_numbers, ids_src)
    kept = slots < CAPACITY
    flat_slot = jnp.where(kept, ids_src * CAPACITY + slots, EXPERTS * CAPACITY)
    token_num = jnp.broadcast_to(jnp.arange(TOKENS, dtype=jnp.int32)[:, None], (TOKENS, TOP))

    def dispatch(operands):
        tok_rows, slot_one = operands
        slot_owner = jnp.full((EXPERTS * CAPACITY + 1,), TOKENS, jnp.int32)
        slot_owner = slot_owner.at[slot_one.reshape(TOKENS * TOP)].set(token_num.reshape(TOKENS * TOP))
        padded = jnp.concatenate([tok_rows, jnp.zeros((1, D), tok_rows.dtype)], axis=0)
        return padded[slot_owner[: EXPERTS * CAPACITY]]

    slot_rows = lax.map(dispatch, (x_src, flat_slot))
    by_expert = slot_rows.reshape(SOURCES, EXPERTS, CAPACITY, D).transpose(1, 0, 2, 3)
    by_expert = by_expert.reshape(EXPERTS, SOURCES * CAPACITY, D)

    def expert_ffn(operands):
        rows_e, wg_e, wu_e, wd_e = operands
        gated = jax.nn.silu(jnp.dot(rows_e, wg_e, preferred_element_type=jnp.float32)) * jnp.dot(rows_e, wu_e, preferred_element_type=jnp.float32)
        hidden = gated.astype(jnp.bfloat16)
        return jnp.dot(hidden, wd_e, preferred_element_type=jnp.float32).astype(jnp.bfloat16)

    y_rows = lax.map(expert_ffn, (by_expert, w_gate, w_up, w_down))
    y_src = y_rows.reshape(EXPERTS, SOURCES, CAPACITY, D).transpose(1, 0, 2, 3)
    y_src = y_src.reshape(SOURCES, EXPERTS * CAPACITY, D)

    def combine(operands):
        y_one, slot_one, gate_one, kept_one = operands
        safe_slot = jnp.minimum(slot_one, EXPERTS * CAPACITY - 1)
        weight = jnp.where(kept_one, gate_one, 0.0)
        total = jnp.zeros((TOKENS, D), jnp.float32)
        for choice in range(TOP):
            total = total + weight[:, choice:choice + 1] * y_one[safe_slot[:, choice]].astype(jnp.float32)
        return total.astype(jnp.bfloat16)

    y_out = lax.map(combine, (y_src, flat_slot, gates_src, kept))
    return y_out.reshape(SOURCES * TOKENS, D)
```

```python
import functools

import jax
import jax.numpy as jnp
from jax import lax
from jax.experimental import pallas as pl
from jax.experimental.pallas import tpu as pltpu
from jax.sharding import PartitionSpec as P

MESH = pl.DeviceIdType.MESH
CAP_NUM = 5
CAP_DEN = 4
GROUP = 4
LEAD = 4
LAG = 6
STEP = 37
F_BLOCK = 512


def moe_kernel(x_ref, ids_ref, gates_ref, wg_hbm, wu_hbm, wd_hbm, o_ref,
               src, arr, ret, wg, wu, wd, pos, g1, g2, g3, onehot, hid, wt, y3, acc, other,
               w_sem, ws_sem, wr_sem, ds_sem, dr_sem, bs_sem, br_sem, xs_sem, xr_sem):
    core = lax.axis_index('tp')
    me = lax.axis_index('ep')
    cx, cy, cz = lax.rem(me, 4), lax.rem(me // 4, 4), me // 16
    tokens, d_model = x_ref.shape
    n_top = ids_ref.shape[0]
    n_groups, rows, _ = src.shape
    share = rows // GROUP
    n_exp = n_groups * GROUP
    half = wg_hbm.shape[2]
    bf16, f32 = jnp.bfloat16, jnp.float32

    def partner(k, sign):
        d = lax.rem(STEP * k, n_exp)
        dx, dy, dz = lax.rem(d, 4), lax.rem(d // 4, 4), d // 16
        if sign < 0:
            dx, dy, dz = 4 - dx, 4 - dy, 4 - dz
        return lax.rem(cx + dx, 4) + 4 * lax.rem(cy + dy, 4) + 16 * lax.rem(cz + dz, 4)

    own = pl.ds(pl.multiple_of(core * half, 128), half)
    spots = ((wg_hbm, wg.at[:, own]), (wu_hbm, wu.at[:, own]), (wd_hbm, wd.at[own, :]))
    local_w, remote_w = [], []
    for i, (hbm, dst) in enumerate(spots):
        local_w.append(pltpu.make_async_copy(hbm.at[0], dst, w_sem.at[i]))
        remote_w.append(pltpu.make_async_remote_copy(
            src_ref=hbm.at[0], dst_ref=dst, send_sem=ws_sem.at[i], recv_sem=wr_sem.at[i],
            device_id={'tp': 1 - core}, device_id_type=MESH))
    for c in local_w + remote_w:
        c.start()

    exp_iota = lax.broadcasted_iota(jnp.int32, (n_exp, 128), 0)
    tri = (lax.broadcasted_iota(jnp.int32, (128, 128), 0)
           < lax.broadcasted_iota(jnp.int32, (128, 128), 1)).astype(f32).astype(bf16)
    before = jnp.zeros((n_exp, 1), f32)
    for b in range(tokens // 128):
        cols = pl.ds(b * 128, 128)
        hot = jnp.zeros((n_exp, 128), f32)
        gate = jnp.zeros((n_exp, 128), f32)
        for j in range(n_top):
            hit = exp_iota == ids_ref[j:j + 1, cols]
            hot = jnp.where(hit, 1.0, hot)
            gate = jnp.where(hit, gates_ref[j:j + 1, cols], gate)
        count = jnp.dot(hot.astype(bf16), tri, preferred_element_type=f32) + before
        pos[:, cols] = jnp.where(hot > 0.0, count, -1.0)
        before = before + jnp.sum(hot, axis=1, keepdims=True)
        p1 = gate.astype(bf16).astype(f32)
        p2 = (gate - p1).astype(bf16).astype(f32)
        g1[:, cols] = p1
        g2[:, cols] = p2
        g3[:, cols] = gate - p1 - p2

    slot_iota = (lax.broadcasted_iota(jnp.int32, (share, tokens), 0) + core * share).astype(f32)

    def send_out(k):
        return pltpu.make_async_remote_copy(
            src_ref=src.at[k // GROUP, pl.ds(pl.multiple_of(lax.rem(k, GROUP) * share, 16), share)],
            dst_ref=arr.at[k // GROUP, pl.ds(pl.multiple_of(lax.rem(k, GROUP) * share, 16), share)],
            send_sem=ds_sem.at[k], recv_sem=dr_sem.at[k],
            device_id={'ep': partner(k, 1)}, device_id_type=MESH)

    def send_back(k):
        return pltpu.make_async_remote_copy(
            src_ref=arr.at[k // GROUP, pl.ds(pl.multiple_of(lax.rem(k, GROUP) * share, 16), share)],
            dst_ref=ret.at[k // GROUP, pl.ds(pl.multiple_of(lax.rem(k, GROUP) * share, 16), share)],
            send_sem=bs_sem.at[k], recv_sem=br_sem.at[k],
            device_id={'ep': partner(k, -1)}, device_id_type=MESH)

    def each(g, fn):
        def one(i, carry):
            k = g * GROUP + i

            @pl.when(k > 0)
            def _():
                fn(k)
            return carry
        lax.fori_loop(0, GROUP, one, 0)

    def dispatch(g):
        for i in range(GROUP):
            row = pos[pl.ds(partner(g * GROUP + i, 1), 1), :]
            onehot[pl.ds(i * share, share), :] = jnp.where(row == slot_iota, 1.0, 0.0).astype(bf16)
        src[g] = jnp.dot(onehot[...], x_ref[...], preferred_element_type=f32).astype(bf16)

        @pl.when(g == 0)
        def _():
            arr[0, 0:share, :] = src[0, 0:share, :]
        each(g, lambda k: send_out(k).start())

    def experts(g):
        each(g, lambda k: send_out(k).wait_recv())

        def block(f, carry):
            cols = pl.ds(pl.multiple_of(f * F_BLOCK, F_BLOCK), F_BLOCK)
            a = jnp.dot(arr[g], wg[:, cols], preferred_element_type=f32)
            b = jnp.dot(arr[g], wu[:, cols], preferred_element_type=f32)
            hid[:, cols] = (a * jax.nn.sigmoid(a) * b).astype(bf16)
            return carry
        lax.fori_loop(0, 2 * half // F_BLOCK, block, 0)
        arr[g] = jnp.dot(hid[...], wd[...], preferred_element_type=f32).astype(bf16)

        @pl.when(g == 0)
        def _():
            ret[0, 0:share, :] = arr[0, 0:share, :]
        each(g, lambda k: send_back(k).start())

    def combine(g, after=None):
        each(g, lambda k: send_back(k).wait_recv())
        for i in range(GROUP):
            e = pl.ds(partner(g * GROUP + i, 1), 1)
            hit = pos[e, :] == slot_iota
            for p, part in enumerate((g1, g2, g3)):
                wt[pl.ds(p * rows + i * share, share), :] = jnp.where(hit, part[e, :], 0.0).astype(bf16)
        for p in range(3):
            y3[pl.ds(p * rows, rows), :] = ret[g]
        for b in range(2):
            blk = pl.ds(b * (tokens // 2), tokens // 2)
            acc[blk, :] += lax.dot_general(wt[:, blk], y3[...], (((0,), (0,)), ((), ())),
                                           preferred_element_type=f32)
            if after is not None:
                after(b)

    def swap(b):
        blk = pl.ds(b * (tokens // 2), tokens // 2)
        return pltpu.make_async_remote_copy(
            src_ref=acc.at[blk], dst_ref=other.at[blk], send_sem=xs_sem.at[b], recv_sem=xr_sem.at[b],
            device_id={'tp': 1 - core}, device_id_type=MESH)

    acc[...] = jnp.zeros_like(acc)

    def ahead(g, carry):
        dispatch(g)
        return carry
    lax.fori_loop(0, LEAD, ahead, 0)
    for c in local_w:
        c.wait()
    for c in remote_w:
        c.wait()

    def step(g, carry):
        @pl.when(g + LEAD < n_groups)
        def _():
            dispatch(g + LEAD)

        @pl.when(g < n_groups)
        def _():
            experts(g)

        @pl.when(g >= LAG)
        def _():
            combine(g - LAG)
        return carry
    lax.fori_loop(0, n_groups + LAG - 1, step, 0)
    combine(n_groups - 1, lambda b: swap(b).start())

    def drain(k, carry):
        send_out(k).wait_send()
        send_back(k).wait_send()
        return carry
    lax.fori_loop(1, n_exp, drain, 0)
    for b in range(2):
        blk = pl.ds(b * (tokens // 2), tokens // 2)
        swap(b).wait()
        o_ref[blk, :] = (acc[blk, :] + other[blk, :]).astype(bf16)


def solution(mesh):
    n_ep = mesh.shape['ep']
    n_tp = mesh.shape['tp']
    row_spec = P(('dp', 'ep'), None)
    vmem = pl.BlockSpec(memory_space=pltpu.VMEM)
    hbm = pl.BlockSpec(memory_space=pl.ANY)

    def device_body(x_loc, ids_loc, gates_loc, wg_loc, wu_loc, wd_loc):
        tokens, d_model = x_loc.shape
        n_top = ids_loc.shape[1]
        n_experts = wg_loc.shape[0] * n_ep
        width = wg_loc.shape[2] * n_tp
        capacity = CAP_NUM * n_top * tokens // (CAP_DEN * n_experts)
        share = capacity // n_tp
        rows, n_groups = GROUP * share, n_experts // GROUP
        bf16, f32 = jnp.bfloat16, jnp.float32
        scratch = [
            pltpu.VMEM((n_groups, rows, d_model), bf16),
            pltpu.VMEM((n_groups, rows, d_model), bf16),
            pltpu.VMEM((n_groups, rows, d_model), bf16),
            pltpu.VMEM((d_model, width), bf16),
            pltpu.VMEM((d_model, width), bf16),
            pltpu.VMEM((width, d_model), bf16),
            pltpu.VMEM((n_experts, tokens), f32),
            pltpu.VMEM((n_experts, tokens), f32),
            pltpu.VMEM((n_experts, tokens), f32),
            pltpu.VMEM((n_experts, tokens), f32),
            pltpu.VMEM((rows, tokens), bf16),
            pltpu.VMEM((rows, width), bf16),
            pltpu.VMEM((3 * rows, tokens), bf16),
            pltpu.VMEM((3 * rows, d_model), bf16),
            pltpu.VMEM((tokens, d_model), f32),
            pltpu.VMEM((tokens, d_model), f32),
            pltpu.SemaphoreType.DMA((3,)),
            pltpu.SemaphoreType.DMA((3,)),
            pltpu.SemaphoreType.DMA((3,)),
            pltpu.SemaphoreType.DMA((n_experts,)),
            pltpu.SemaphoreType.DMA((n_experts,)),
            pltpu.SemaphoreType.DMA((n_experts,)),
            pltpu.SemaphoreType.DMA((n_experts,)),
            pltpu.SemaphoreType.DMA((2,)),
            pltpu.SemaphoreType.DMA((2,)),
        ]
        return pl.pallas_call(
            moe_kernel,
            out_shape=jax.ShapeDtypeStruct((tokens, d_model), bf16),
            in_specs=[vmem, vmem, vmem, hbm, hbm, hbm],
            out_specs=vmem,
            scratch_shapes=scratch,
            compiler_params=pltpu.CompilerParams(has_side_effects=True, vmem_limit_bytes=67043328),
        )(x_loc, ids_loc.T, gates_loc.T, wg_loc, wu_loc, wd_loc)

    return jax.shard_map(device_body, mesh=mesh,
                         in_specs=(row_spec, row_spec, row_spec, P('ep', None, 'tp'), P('ep', None, 'tp'), P('ep', 'tp', None)),
                         out_specs=row_spec, check_vma=False)
```

```python
import functools

import jax
import jax.numpy as jnp
from jax import lax
from jax.experimental import pallas as pl
from jax.experimental.pallas import tpu as pltpu
from jax.sharding import PartitionSpec as P

MESH = pl.DeviceIdType.MESH
CAP_NUM = 5
CAP_DEN = 4
PARTS = (32, 32, 16)
LEAD = 6
LAGS = (0, 2, 4, 6, 8, 10)
SIDE = 4
F_BLOCK = 512


def moe_kernel(x_ref, ids_ref, gates_ref, wg_hbm, wu_hbm, wd_hbm, o_ref, r1, r2, r4, r5,
               src, arr, ret, wg, wu, wd, pos, g1, g2, g3, onehot, hid, wt, y3, acc, other,
               w_sem, ws_sem, wr_sem, p1s, p1r, q1s, q1r, p2s, p2r, p3s, p3r, q3s, q3r, q2s, q2r,
               out_sem, in_sem, xs_sem, xr_sem):
    core = lax.axis_index('tp')
    me = lax.axis_index('ep')
    here = (lax.rem(me, SIDE), lax.rem(me // SIDE, SIDE), me // (SIDE * SIDE))
    tokens, d_model = x_ref.shape
    n_top = ids_ref.shape[0]
    n_chunks, rows, _ = src.shape
    share = rows // SIDE
    n_exp = n_chunks * SIDE
    half = wg_hbm.shape[2]
    bf16, f32 = jnp.bfloat16, jnp.float32
    colors = range(len(PARTS))
    first = [SIDE * sum(PARTS[:r]) for r in colors]

    def device(r, d, sign):
        e = d if sign > 0 else tuple(SIDE - v for v in d)
        out = 0
        for axis, scale in ((0, 1), (1, SIDE), (2, SIDE * SIDE)):
            v0, v1 = e[(axis - r) % 3], e[(axis - r - 1) % 3]
            out = out + scale * lax.rem(here[axis] + v0 + core * (v1 - v0), SIDE)
        return out

    def offs(c):
        db = lax.rem(c, SIDE)
        return db, lax.rem(db + c // SIDE, SIDE)

    def piece(r, da):
        return pl.ds(first[r] + da * PARTS[r], PARTS[r])

    def block(r):
        return pl.ds(first[r], SIDE * PARTS[r])

    def remote(a, b, s_sem, r_sem, dev):
        return pltpu.make_async_remote_copy(src_ref=a, dst_ref=b, send_sem=s_sem, recv_sem=r_sem,
                                            device_id={'ep': dev}, device_id_type=MESH)

    def p1(r, c, da, dst):
        return remote(src.at[c, piece(r, da)], dst.at[c, piece(r, da)], p1s.at[r, c, da - 1], p1r.at[r, c, da - 1],
                      device(r, (da, 0, 0), 1))

    def p2(r, c, dst):
        return remote(r1.at[c, block(r)], dst.at[c, block(r)], p2s.at[r, c], p2r.at[r, c],
                      device(r, (0, offs(c)[0], 0), 1))

    def p3(r, c, a):
        return remote(a.at[c, block(r)], arr.at[c, block(r)], p3s.at[r, c], p3r.at[r, c],
                      device(r, (0, 0, offs(c)[1]), 1))

    def q3(r, c, dst):
        return remote(arr.at[c, block(r)], dst.at[c, block(r)], q3s.at[r, c], q3r.at[r, c],
                      device(r, (0, 0, offs(c)[1]), -1))

    def q2(r, c, a):
        return remote(a.at[c, block(r)], r5.at[c, block(r)], q2s.at[r, c], q2r.at[r, c],
                      device(r, (0, offs(c)[0], 0), -1))

    def q1(r, c, da, a):
        return remote(a.at[c, piece(r, da)], ret.at[c, piece(r, da)], q1s.at[r, c, da - 1], q1r.at[r, c, da - 1],
                      device(r, (da, 0, 0), -1))

    def own_out(r, c):
        return pltpu.make_async_copy(src.at[c, piece(r, 0)], r1.at[c, piece(r, 0)], out_sem.at[r, c])

    def own_in(r, c):
        return pltpu.make_async_copy(r5.at[c, piece(r, 0)], ret.at[c, piece(r, 0)], in_sem.at[r, c])

    own = pl.ds(pl.multiple_of(core * half, 128), half)
    spots = ((wg_hbm, wg.at[:, own]), (wu_hbm, wu.at[:, own]), (wd_hbm, wd.at[own, :]))
    local_w, remote_w = [], []
    for i, (hbm, dst) in enumerate(spots):
        local_w.append(pltpu.make_async_copy(hbm.at[0], dst, w_sem.at[i]))
        remote_w.append(pltpu.make_async_remote_copy(
            src_ref=hbm.at[0], dst_ref=dst, send_sem=ws_sem.at[i], recv_sem=wr_sem.at[i],
            device_id={'tp': 1 - core}, device_id_type=MESH))
    for c in local_w + remote_w:
        c.start()

    exp_iota = lax.broadcasted_iota(jnp.int32, (n_exp, 128), 0)
    tri = (lax.broadcasted_iota(jnp.int32, (128, 128), 0)
           < lax.broadcasted_iota(jnp.int32, (128, 128), 1)).astype(f32).astype(bf16)
    before = jnp.zeros((n_exp, 1), f32)
    for b in range(tokens // 128):
        cols = pl.ds(b * 128, 128)
        hot = jnp.zeros((n_exp, 128), f32)
        gate = jnp.zeros((n_exp, 128), f32)
        for j in range(n_top):
            hit = exp_iota == ids_ref[j:j + 1, cols]
            hot = jnp.where(hit, 1.0, hot)
            gate = jnp.where(hit, gates_ref[j:j + 1, cols], gate)
        count = jnp.dot(hot.astype(bf16), tri, preferred_element_type=f32) + before
        pos[:, cols] = jnp.where(hot > 0.0, count, -1.0)
        before = before + jnp.sum(hot, axis=1, keepdims=True)
        part1 = gate.astype(bf16).astype(f32)
        part2 = (gate - part1).astype(bf16).astype(f32)
        g1[:, cols] = part1
        g2[:, cols] = part2
        g3[:, cols] = gate - part1 - part2

    def slots(r):
        start = core * share + sum(PARTS[:r])
        return (lax.broadcasted_iota(jnp.int32, (PARTS[r], tokens), 0) + start).astype(f32)

    def send_out(c):
        db, dc = offs(c)
        for r in colors:
            want = slots(r)
            for da in range(SIDE):
                row = pos[pl.ds(device(r, (da, db, dc), 1), 1), :]
                onehot[piece(r, da), :] = jnp.where(row == want, 1.0, 0.0).astype(bf16)
        src[c] = jnp.dot(onehot[...], x_ref[...], preferred_element_type=f32).astype(bf16)

        @pl.when(c == 0)
        def _():
            for r in colors:
                arr[0, piece(r, 0), :] = src[0, piece(r, 0), :]
                for da in (2, 1, 3):
                    p1(r, c, da, arr).start()

        @pl.when(c > 0)
        def _():
            for r in colors:
                own_out(r, c).start()
                for da in (2, 1, 3):
                    p1(r, c, da, r1).start()

    def relay_b(c):
        db, dc = offs(c)

        @pl.when(c == 0)
        def _():
            for r in colors:
                for da in (1, 2, 3):
                    p1(r, c, da, arr).wait_recv()

        @pl.when(c > 0)
        def _():
            for r in colors:
                own_out(r, c).wait()
                for da in (1, 2, 3):
                    p1(r, c, da, r1).wait_recv()

        @pl.when((db > 0) & (dc == 0))
        def _():
            for r in colors:
                p2(r, c, arr).start()

        @pl.when((db > 0) & (dc > 0))
        def _():
            for r in colors:
                p2(r, c, r2).start()

        @pl.when((db == 0) & (dc > 0))
        def _():
            for r in colors:
                p3(r, c, r1).start()

    def relay_c(c):
        db, dc = offs(c)

        @pl.when((db > 0) & (dc > 0))
        def _():
            for r in colors:
                p2(r, c, r2).wait_recv()
                p3(r, c, r2).start()

    def experts(c):
        db, dc = offs(c)

        @pl.when((db > 0) & (dc == 0))
        def _():
            for r in colors:
                p2(r, c, arr).wait_recv()

        @pl.when(dc > 0)
        def _():
            for r in colors:
                p3(r, c, r2).wait_recv()

        def part(f, carry):
            cols = pl.ds(pl.multiple_of(f * F_BLOCK, F_BLOCK), F_BLOCK)
            a = jnp.dot(arr[c], wg[:, cols], preferred_element_type=f32)
            b = jnp.dot(arr[c], wu[:, cols], preferred_element_type=f32)
            hid[:, cols] = (a * jax.nn.sigmoid(a) * b).astype(bf16)
            return carry
        lax.fori_loop(0, 2 * half // F_BLOCK, part, 0)
        arr[c] = jnp.dot(hid[...], wd[...], preferred_element_type=f32).astype(bf16)

        @pl.when((db > 0) & (dc > 0))
        def _():
            for r in colors:
                q3(r, c, r4).start()

        @pl.when((db == 0) & (dc > 0))
        def _():
            for r in colors:
                q3(r, c, r5).start()

        @pl.when((db > 0) & (dc == 0))
        def _():
            for r in colors:
                q2(r, c, arr).start()

        @pl.when(c == 0)
        def _():
            for r in colors:
                ret[0, piece(r, 0), :] = arr[0, piece(r, 0), :]
                for da in (2, 1, 3):
                    q1(r, c, da, arr).start()

    def back_b(c):
        db, dc = offs(c)

        @pl.when((db > 0) & (dc > 0))
        def _():
            for r in colors:
                q3(r, c, r4).wait_recv()
                q2(r, c, r4).start()

    def back_a(c):
        db, dc = offs(c)

        @pl.when((db == 0) & (dc > 0))
        def _():
            for r in colors:
                q3(r, c, r5).wait_recv()

        @pl.when(db > 0)
        def _():
            for r in colors:
                q2(r, c, r4).wait_recv()

        @pl.when(c > 0)
        def _():
            for r in colors:
                own_in(r, c).start()
                for da in (2, 1, 3):
                    q1(r, c, da, r5).start()

    def combine(c, after=None):
        db, dc = offs(c)
        for r in colors:
            for da in (1, 2, 3):
                q1(r, c, da, r5).wait_recv()

        @pl.when(c > 0)
        def _():
            for r in colors:
                own_in(r, c).wait()
        for r in colors:
            want = slots(r)
            for da in range(SIDE):
                e = pl.ds(device(r, (da, db, dc), 1), 1)
                hit = pos[e, :] == want
                for p, part in enumerate((g1, g2, g3)):
                    wt[pl.ds(p * rows + first[r] + da * PARTS[r], PARTS[r]), :] = (
                        jnp.where(hit, part[e, :], 0.0).astype(bf16))
        for p in range(3):
            y3[pl.ds(p * rows, rows), :] = ret[c]
        for b in range(2):
            blk = pl.ds(b * (tokens // 2), tokens // 2)
            acc[blk, :] += lax.dot_general(wt[:, blk], y3[...], (((0,), (0,)), ((), ())),
                                           preferred_element_type=f32)
            if after is not None:
                after(b)

    def swap(b):
        blk = pl.ds(b * (tokens // 2), tokens // 2)
        return pltpu.make_async_remote_copy(
            src_ref=acc.at[blk], dst_ref=other.at[blk], send_sem=xs_sem.at[b], recv_sem=xr_sem.at[b],
            device_id={'tp': 1 - core}, device_id_type=MESH)

    acc[...] = jnp.zeros_like(acc)

    def ahead(c, carry):
        send_out(c)
        return carry
    lax.fori_loop(0, LEAD, ahead, 0)
    for c in local_w:
        c.wait()
    for c in remote_w:
        c.wait()

    def step(t, carry):
        def at(c, fn):
            @pl.when((c >= 0) & (c < n_chunks))
            def _():
                fn(c)
        at(t + LEAD, send_out)
        at(t - LAGS[4], back_a)
        at(t - LAGS[3], back_b)
        at(t - LAGS[1], relay_c)
        at(t - LAGS[0], relay_b)
        at(t - LAGS[2], experts)

        @pl.when((t >= LAGS[5]))
        def _():
            combine(t - LAGS[5])
        return carry
    lax.fori_loop(0, n_chunks + LAGS[5] - 1, step, 0)
    combine(n_chunks - 1, lambda b: swap(b).start())

    def drain(c, carry):
        db, dc = offs(c)
        for r in colors:
            for da in (1, 2, 3):
                p1(r, c, da, r1).wait_send()
                q1(r, c, da, r5).wait_send()

        @pl.when(db > 0)
        def _():
            for r in colors:
                p2(r, c, r2).wait_send()
                q2(r, c, r4).wait_send()

        @pl.when(dc > 0)
        def _():
            for r in colors:
                p3(r, c, r2).wait_send()
                q3(r, c, r4).wait_send()
        return carry
    lax.fori_loop(0, n_chunks, drain, 0)
    for b in range(2):
        blk = pl.ds(b * (tokens // 2), tokens // 2)
        swap(b).wait()
        o_ref[blk, :] = (acc[blk, :] + other[blk, :]).astype(bf16)


def solution(mesh):
    n_ep = mesh.shape['ep']
    n_tp = mesh.shape['tp']
    row_spec = P(('dp', 'ep'), None)
    vmem = pl.BlockSpec(memory_space=pltpu.VMEM)
    hbm = pl.BlockSpec(memory_space=pl.ANY)

    def device_body(x_loc, ids_loc, gates_loc, wg_loc, wu_loc, wd_loc):
        tokens, d_model = x_loc.shape
        n_top = ids_loc.shape[1]
        n_experts = wg_loc.shape[0] * n_ep
        width = wg_loc.shape[2] * n_tp
        capacity = CAP_NUM * n_top * tokens // (CAP_DEN * n_experts)
        share = capacity // n_tp
        rows, n_groups = SIDE * share, n_experts // SIDE
        bf16, f32 = jnp.bfloat16, jnp.float32
        scratch = [
            pltpu.VMEM((n_groups, rows, d_model), bf16),
            pltpu.VMEM((n_groups, rows, d_model), bf16),
            pltpu.VMEM((n_groups, rows, d_model), bf16),
            pltpu.VMEM((d_model, width), bf16),
            pltpu.VMEM((d_model, width), bf16),
            pltpu.VMEM((width, d_model), bf16),
            pltpu.VMEM((n_experts, tokens), f32),
            pltpu.VMEM((n_experts, tokens), f32),
            pltpu.VMEM((n_experts, tokens), f32),
            pltpu.VMEM((n_experts, tokens), f32),
            pltpu.VMEM((rows, tokens), bf16),
            pltpu.VMEM((rows, width), bf16),
            pltpu.VMEM((3 * rows, tokens), bf16),
            pltpu.VMEM((3 * rows, d_model), bf16),
            pltpu.VMEM((tokens, d_model), f32),
            pltpu.VMEM((tokens, d_model), f32),
            pltpu.SemaphoreType.DMA((3,)),
            pltpu.SemaphoreType.DMA((3,)),
            pltpu.SemaphoreType.DMA((3,)),
            pltpu.SemaphoreType.DMA((len(PARTS), n_groups, SIDE - 1)),
            pltpu.SemaphoreType.DMA((len(PARTS), n_groups, SIDE - 1)),
            pltpu.SemaphoreType.DMA((len(PARTS), n_groups, SIDE - 1)),
            pltpu.SemaphoreType.DMA((len(PARTS), n_groups, SIDE - 1)),
            pltpu.SemaphoreType.DMA((len(PARTS), n_groups)),
            pltpu.SemaphoreType.DMA((len(PARTS), n_groups)),
            pltpu.SemaphoreType.DMA((len(PARTS), n_groups)),
            pltpu.SemaphoreType.DMA((len(PARTS), n_groups)),
            pltpu.SemaphoreType.DMA((len(PARTS), n_groups)),
            pltpu.SemaphoreType.DMA((len(PARTS), n_groups)),
            pltpu.SemaphoreType.DMA((len(PARTS), n_groups)),
            pltpu.SemaphoreType.DMA((len(PARTS), n_groups)),
            pltpu.SemaphoreType.DMA((len(PARTS), n_groups)),
            pltpu.SemaphoreType.DMA((len(PARTS), n_groups)),
            pltpu.SemaphoreType.DMA((2,)),
            pltpu.SemaphoreType.DMA((2,)),
        ]
        return pl.pallas_call(
            moe_kernel,
            out_shape=[jax.ShapeDtypeStruct((tokens, d_model), bf16)]
            + [jax.ShapeDtypeStruct((n_groups, rows, d_model), bf16)] * 4,
            in_specs=[vmem, vmem, vmem, hbm, hbm, hbm],
            out_specs=[vmem, hbm, hbm, hbm, hbm],
            scratch_shapes=scratch,
            compiler_params=pltpu.CompilerParams(has_side_effects=True, vmem_limit_bytes=67043328),
        )(x_loc, ids_loc.T, gates_loc.T, wg_loc, wu_loc, wd_loc)[0]

    return jax.shard_map(device_body, mesh=mesh,
                         in_specs=(row_spec, row_spec, row_spec, P('ep', None, 'tp'), P('ep', None, 'tp'), P('ep', 'tp', None)),
                         out_specs=row_spec, check_vma=False)
```
